128 devices in a mesh: gx: 16 (over y, x), gy: 8 (over z, core).
Axes of the slice: x: 4, y: 4, z: 4, core: 2. Of those that a mesh axis runs over, the one named last changes fastest.
Arguments:
- point_feats: bfloat16 [1048576, 128], P(('gx', 'gy')), may hold values from -6 to 6
- point_tile: int32 [1048576, 1], P(('gx', 'gy')), may hold values from 0 to 127; in each aligned block of 8192 rows (0 to 8191, 8192 to 16383, ...) at most 80 rows name the same one
- point_cell: int32 [1048576], P(('gx', 'gy')), may hold values from 0 to 4095
- point_count: int32 [128], P(('gx', 'gy')), may hold values from 6144 to 8192, as said below
- conv_weight: bfloat16 [3, 3, 128, 128], replicated, may hold values from -0.1875 to 0.1875
- conv_bias: float32 [128], replicated, may hold values from -3 to 3
Outputs:
- bev_map: bfloat16 [256, 2048, 128], P('gx', 'gy')
- conv_out: bfloat16 [256, 2048, 128], P('gx', 'gy')
The draws below stay inside these ranges and needn't reach their ends.
Inputs may be any that keep to these rules, and one draw needn't show every extreme that they name: `point_tile`: among the 8192 rows of one device no tile is named by more than 80 rows, a bound that some block reaches. `point_count`: only slots below a device's count are live; some device has all 8192 slots live.
All inputs are finite; a program needn't handle non-finite values.
Results may differ from the reference program's by a relative error of at most 0.0045.
Values may be sent and summed in bfloat16 or wider, within the bound.
A program may use at most 64 MiB of HBM per device.

```python
import math
import jax
import jax.numpy as jnp
import numpy as np
from jax import lax

C = 128
COLS_DEV = 256
ROWS_DEV = 16
P_DEV = 8192
CAP = 80
POINTS = 1048576
MAP_ROWS = 256
MAP_COLS = 2048
N_GY = 8
DEVICES = 128


def draw_point_count(key, part):
    counts = jax.random.randint(key, (DEVICES,), 3 * P_DEV // 4, P_DEV + 1).astype(jnp.int32)
    fullest = jax.random.randint(jax.random.fold_in(key, 7), (), 0, DEVICES)
    return counts.at[fullest].set(P_DEV)


def with_ends(array, key, low, high):
    longest = array.shape.index(max(array.shape))
    spots = []
    for shift in (0, 1):
        where = [jax.random.randint(jax.random.fold_in(key, axis), (), 0, length) for axis, length in enumerate(array.shape)]
        where[longest] = (where[longest] + shift) % array.shape[longest]
        spots.append(tuple(where))
    return array.at[spots[0]].set(low).at[spots[1]].set(high)


def level_of(own_key, dims, cuts, low, largest):
    loudness, own = 1.0, jax.random.fold_in(own_key, 6)
    for dim, blocks in cuts:
        steps = jnp.exp(jax.random.uniform(jax.random.fold_in(own, dim), (blocks,), jnp.float32, low / len(cuts), largest / len(cuts)))
        loudness = loudness * jnp.repeat(steps, dims[dim] // blocks).reshape([-1 if axis == dim else 1 for axis in range(len(dims))])
    return loudness


def routed_block(own_key, own, number, rows, count, top, most, slope):
    sequence = jax.random.permutation(own_key, count)
    packed, usual = load_shares(count, rows * top, most, slope, True), load_shares(count, rows * top, most, slope, False)
    places = jnp.arange(count)

    def named(lengths, rotation):
        used = int((lengths > 0).sum())
        fixed = max(1, used // 4)
        passed = fixed + (places - fixed + rotation * (used - fixed)) % max(1, count - fixed)
        return jnp.zeros((count,), jnp.int32).at[sequence[jnp.where(places < fixed, places, passed)]].set(jnp.asarray(lengths, jnp.int32))

    lengths = jnp.where(number % 4 == 0, named(packed, number // 4), named(usual, number - number // 4 - 1))
    mixed = jax.random.permutation(jax.random.fold_in(own, 3), count)
    source_of, sink = mixed[0:count // 2 * 2:2], mixed[1:count // 2 * 2:2]
    margin = jnp.minimum(lengths[source_of] - 1, most - lengths[sink]) // 2
    margin = jnp.where((source_of == sequence[0]) | (sink == sequence[0]) | (lengths[sink] == 0), 0, jnp.maximum(margin, 0))
    passed = jax.random.randint(jax.random.fold_in(own, 4), (count // 2,), 0, 1 << 20) % (margin + 1)
    lengths = lengths.at[source_of].add(-passed).at[sink].add(passed)
    labels = jnp.searchsorted(jnp.cumsum(lengths), jnp.arange(rows * top), side="right").astype(jnp.int32)
    grid = labels.reshape(top, rows).T
    grid = grid[jax.random.permutation(jax.random.fold_in(own, 1), rows)]
    rotation = jax.random.randint(jax.random.fold_in(own, 2), (rows, 1), 0, top)
    return jnp.take_along_axis(grid, (jnp.arange(top)[None, :] + rotation) % top, axis=1)


def load_shares(number_of, total, bound, lean, full):
    loads = [(1 << 20) // math.isqrt(grade ** lean) + 1 for grade in range(1, number_of + 1)]
    largest = bound if full else min(bound, max(-(-total // number_of), total * loads[0] // sum(loads)))
    least = 1 if total - largest >= number_of - 1 else 0
    holding, spare = [largest] + [least] * (number_of - 1), total - largest - least * (number_of - 1)
    while spare > 0:
        candidates = [i for i in range(1, number_of) if holding[i] < largest] or [i for i in range(1, number_of) if holding[i] < bound]
        pool, left = sum([loads[i] for i in candidates]), spare
        for i in candidates:
            more = min(bound - holding[i], max(1, left * loads[i] // pool), spare)
            holding[i] = holding[i] + more
            spare = spare - more
    return np.array(holding)


def scatter_about(own_key, dims, deviation, reach, cuts=(), kind=jnp.bfloat16):
    drawn = jax.random.normal(own_key, dims, jnp.float32) * deviation
    if len(cuts) > 0:
        drawn = level_of(own_key, dims, cuts, -0.22, 0.18) * drawn
    return jnp.clip(drawn, min=-reach, max=reach).astype(kind)


def setup_inputs(seed: int = 0) -> dict:
    seeds = jax.random.split(jax.random.key(seed), 7)
    point_feats = scatter_about(seeds[0], (POINTS, C), 1.0, 6.0, ((0, 128),))
    point_tile_keys = jax.random.split(jax.random.fold_in(seeds[1], 1), POINTS // P_DEV)
    point_tile_turns = jax.random.permutation(jax.random.fold_in(seeds[1], 3), POINTS // P_DEV)
    point_tile = jax.vmap(lambda own, number: routed_block(jax.random.fold_in(seeds[1], 2), own, number, P_DEV, DEVICES, 1, CAP, 2))(point_tile_keys, point_tile_turns).reshape((POINTS, 1))
    point_cell = with_ends(jax.random.randint(seeds[2], (POINTS,), 0, ROWS_DEV * COLS_DEV), jax.random.fold_in(seeds[2], 1), 0, (ROWS_DEV * COLS_DEV) - 1).astype(jnp.int32)
    point_count = draw_point_count(jax.random.fold_in(seeds[6], 71), 0)
    conv_weight = scatter_about(seeds[4], (3, 3, C, C), (9 * C) ** -0.5, 0.1875)
    conv_bias = scatter_about(seeds[5], (C,), 0.5, 3.0, (), jnp.float32)
    return dict(point_feats=point_feats, point_tile=point_tile, point_cell=point_cell, point_count=point_count, conv_weight=conv_weight, conv_bias=conv_bias)


def reference(point_feats, point_tile, point_cell, point_count, conv_weight, conv_bias):
    tile = point_tile[:, 0]
    rows = (tile // N_GY) * ROWS_DEV + point_cell // COLS_DEV
    cols = (tile % N_GY) * COLS_DEV + point_cell % COLS_DEV
    cell = rows * MAP_COLS + cols
    slot = jnp.arange(POINTS, dtype=jnp.int32)
    block = slot // P_DEV
    live = (slot % P_DEV) < point_count[block]
    feats = jnp.where(live[:, None], point_feats.astype(jnp.float32), 0.0)
    sums = jax.ops.segment_sum(feats, cell, num_segments=MAP_ROWS * MAP_COLS)
    bev_map = sums.reshape(MAP_ROWS, MAP_COLS, C).astype(jnp.bfloat16)
    conv = lax.conv_general_dilated(bev_map.astype(jnp.float32)[None], conv_weight.astype(jnp.float32), (1, 1), "SAME", dimension_numbers=("NHWC", "HWIO", "NHWC"), precision=lax.Precision.HIGHEST)[0]
    conv_out = jax.nn.relu(conv + conv_bias).astype(jnp.bfloat16)
    return bev_map, conv_out
```

```python
import functools

import jax
import jax.numpy as jnp
from jax import lax
from jax.experimental import pallas as pl
from jax.experimental.pallas import tpu as pltpu
from jax.sharding import PartitionSpec as P

MESH = pl.DeviceIdType.MESH
F32 = jnp.float32
BF16 = jnp.bfloat16
C = 128
COLS = 256
ROWS = 16
POINTS = 8192
CAP = 80
DEV = 128
GROUP = 16
GROUPS = DEV // GROUP
SPAN = GROUP * CAP
STRIDE = 45
BLOCK = 512


def iota(shape, dim):
    return lax.broadcasted_iota(jnp.int32, shape, dim)


def index_kernel(tile_ref, cell_ref, count_ref, inv_ref, send_cell_ref, offs, table):
    offs[...] = jnp.zeros_like(offs)
    table[...] = jnp.zeros_like(table)
    upper = (iota((BLOCK, BLOCK), 0) <= iota((BLOCK, BLOCK), 1)).astype(BF16)
    ones = jnp.ones((BLOCK, 128), BF16)
    count = count_ref[0]

    def step(b, carry):
        tile = tile_ref[pl.ds(b, 1), :]
        cell = cell_ref[pl.ds(b, 1), :]
        p = b * BLOCK + iota((1, BLOCK), 1)
        tile = jnp.where(p < count, tile, DEV)
        hit = iota((DEV, BLOCK), 0) == tile
        hit16 = hit.astype(F32).astype(BF16)
        cum = jnp.dot(hit16, upper, preferred_element_type=F32)
        base = jnp.concatenate([offs[...]] * (BLOCK // 128), axis=1)
        rank = jnp.sum(jnp.where(hit, cum + base, 0.0), axis=0, keepdims=True) - 1.0
        offs[...] += jnp.dot(hit16, ones, preferred_element_type=F32)
        slot = iota((128, BLOCK), 0).astype(F32) == rank
        parts = []
        for value in ((p >> 8) + 1, p & 255, cell >> 8, cell & 255):
            parts.append(jnp.where(slot, value.astype(F32), 0.0).astype(BF16))
        table[...] += lax.dot_general(
            hit16,
            jnp.concatenate(parts, axis=0),
            (((1,), (1,)), ((), ())),
            preferred_element_type=F32,
        )
        return carry

    lax.fori_loop(0, POINTS // BLOCK, step, 0)
    high = table[:, 0:128]
    filled = high > 0.0
    source = (high - 1.0) * 256.0 + table[:, 128:256]
    inv_ref[...] = jnp.where(filled, source, float(POINTS)).astype(jnp.int32)
    send_cell_ref[...] = jnp.where(filled, table[:, 256:384] * 256.0 + table[:, 384:512], -1.0)


def place():
    gx = lax.axis_index("gx")
    gy = lax.axis_index("gy")
    return lax.rem(gx, 4), lax.div(gx, 4), lax.div(gy, 2), lax.rem(gy, 2)


def partner(i):
    x, y, z, c = place()
    o = lax.rem(i * STRIDE, DEV)
    tc = lax.rem(c + lax.rem(o, 2), 2)
    tz = lax.rem(z + lax.rem(lax.div(o, 2), 4), 4)
    tx = lax.rem(x + lax.rem(lax.div(o, 8), 4), 4)
    ty = lax.rem(y + lax.div(o, 32), 4)
    return ty * 4 + tx, tz * 2 + tc


def main_kernel(
    inv_ref, feats_ref, cell_ref, w_ref, bias_ref, bev_ref, conv_ref,
    src, stage, send, recv, cells_in, acc, expand, onehot, row_bc, xs, wmat, bev, top, bottom,
    col_send, col_recv, corner_send, corner_recv, ext, edge, stage_col,
    send_sem, cell_send_sem, recv_sem, cell_sem, halo_send_sem, halo_sem,
):
    gx = lax.axis_index("gx")
    gy = lax.axis_index("gy")
    zero_row = jnp.zeros((COLS, C), BF16)
    top[...] = zero_row
    bottom[...] = zero_row
    col_recv[...] = jnp.zeros_like(col_recv)
    corner_recv[...] = jnp.zeros_like(corner_recv)

    barrier = pltpu.get_barrier_semaphore()

    def greet(i, carry):
        pl.semaphore_signal(barrier, inc=1, device_id=partner(i), device_id_type=MESH)
        return carry

    lax.fori_loop(1, DEV, greet, 0)

    def widen(b, carry):
        at = pl.multiple_of(b * 256, 256)
        src[pl.ds(at, 256), :] = feats_ref[pl.ds(at, 256), :].astype(F32)
        return carry

    lax.fori_loop(0, POINTS // 256, widen, 0)
    src[pl.ds(POINTS, 8), :] = jnp.zeros((8, C), F32)
    for a in range(3):
        for b in range(3):
            wmat[a * C : (a + 1) * C, b * C : (b + 1) * C] = w_ref[a, b]
    acc[...] = jnp.zeros_like(acc)
    lane = iota((1, SPAN), 1).astype(F32)
    owner = jnp.floor((lane + 0.5) * (1.0 / CAP))
    within = lane - owner * CAP
    expand[...] = (iota((128, SPAN), 0).astype(F32) == within).astype(F32).astype(BF16)

    pl.semaphore_wait(barrier, DEV - 1)

    def cell_copy(i, dest):
        return pltpu.make_async_remote_copy(
            src_ref=cell_ref.at[dest[0] * 8 + dest[1]],
            dst_ref=cells_in.at[i],
            send_sem=cell_send_sem,
            recv_sem=cell_sem.at[lax.div(i, GROUP)],
            device_id=dest,
            device_id_type=MESH,
        )

    def feat_copy(i):
        return pltpu.make_async_remote_copy(
            src_ref=send.at[i],
            dst_ref=recv.at[i],
            send_sem=send_sem,
            recv_sem=recv_sem.at[lax.div(i, GROUP)],
            device_id=partner(i),
            device_id_type=MESH,
        )

    def send_cells(i, carry):
        cell_copy(i, partner(i)).start()
        return carry

    lax.fori_loop(1, DEV, send_cells, 0)

    def pack(tile):
        for k in range(CAP):
            stage[k : k + 1, :] = src[pl.ds(inv_ref[tile, k], 1), :]
        return stage[...].astype(BF16)

    own = gx * 8 + gy
    recv[0] = pack(own)
    cells_in[0] = cell_ref[own]

    def pack_and_send(i, carry):
        dest = partner(i)
        send[i] = pack(dest[0] * 8 + dest[1])

        @pl.when(i > 1)
        def _():
            feat_copy(i - 1).start()

        return carry

    lax.fori_loop(1, DEV, pack_and_send, 0)
    feat_copy(DEV - 1).start()

    eye = iota((128, 128), 0) == iota((128, 128), 1)
    ones = jnp.ones((128, 128), BF16)
    mine = iota((GROUP, SPAN), 0).astype(F32) == owner

    def scatter(g):
        for j in range(GROUP):
            xs[j : j + 1, :] = cells_in[g * GROUP + j]
        cell = xs[...]
        row = jnp.floor(cell * (1.0 / COLS))
        col = cell - row * COLS
        both = jnp.concatenate([row, col], axis=0).astype(BF16)
        dense = jnp.dot(both, expand[...], preferred_element_type=F32)
        row_line = jnp.sum(jnp.where(mine, dense[0:GROUP], 0.0), axis=0, keepdims=True)
        col_line = jnp.sum(jnp.where(mine, dense[GROUP:], 0.0), axis=0, keepdims=True)
        onehot[...] = (iota((COLS, SPAN), 0).astype(F32) == col_line).astype(F32).astype(BF16)
        for q in range(SPAN // 128):
            span = slice(q * 128, (q + 1) * 128)
            diag = jnp.where(eye, row_line[:, span], 0.0).astype(BF16)
            row_bc[span, :] = jnp.dot(diag, ones, preferred_element_type=F32).astype(BF16)
        feats = recv[pl.ds(pl.multiple_of(g * GROUP, GROUP), GROUP)].reshape(SPAN, C)
        rows = row_bc[...]
        none = jnp.zeros((), BF16)
        for pair in range(ROWS // 2):
            even = jnp.where(rows == jnp.asarray(2 * pair, BF16), feats, none)
            odd = jnp.where(rows == jnp.asarray(2 * pair + 1, BF16), feats, none)
            acc[pair] += jnp.dot(
                onehot[...], jnp.concatenate([even, odd], axis=1), preferred_element_type=F32
            )

    def landed(g, first):
        at = pl.ds(g * GROUP + first, GROUP - first)
        pltpu.make_async_copy(cells_in.at[at], cells_in.at[at], cell_sem.at[g]).wait()
        pltpu.make_async_copy(recv.at[at], recv.at[at], recv_sem.at[g]).wait()

    landed(0, 1)
    scatter(0)

    def absorb(g, carry):
        landed(g, 0)
        scatter(g)
        return carry

    lax.fori_loop(1, GROUPS, absorb, 0)

    for r in range(ROWS):
        half = slice((r % 2) * C, (r % 2 + 1) * C)
        line = acc[r // 2, :, half]
        rounded = line.astype(BF16)
        bev[r] = rounded
        bev_ref[r] = rounded
        stage_col[0, r : r + 1, :] = line[0:1, :]
        stage_col[1, r : r + 1, :] = line[COLS - 1 : COLS, :]
    col_send[0] = stage_col[0].astype(BF16)
    col_send[1] = stage_col[1].astype(BF16)
    for k in range(4):
        at = (ROWS - 1) * (k // 2)
        corner_send[k] = jnp.broadcast_to(stage_col[k % 2, at : at + 1, :], (16, C)).astype(BF16)

    def halo(source, target, k, dx, dy):
        return pltpu.make_async_remote_copy(
            src_ref=source,
            dst_ref=target,
            send_sem=halo_send_sem.at[k],
            recv_sem=halo_sem.at[k],
            device_id=(gx + dx, gy + dy),
            device_id_type=MESH,
        )

    moves = [
        (bev.at[0], bottom, -1, 0),
        (bev.at[ROWS - 1], top, 1, 0),
        (col_send.at[0], col_recv.at[1], 0, -1),
        (col_send.at[1], col_recv.at[0], 0, 1),
        (corner_send.at[0], corner_recv.at[3], -1, -1),
        (corner_send.at[1], corner_recv.at[2], -1, 1),
        (corner_send.at[2], corner_recv.at[1], 1, -1),
        (corner_send.at[3], corner_recv.at[0], 1, 1),
    ]

    def inside(dx, dy):
        fine = jnp.logical_and(gx + dx >= 0, gx + dx < 16)
        return jnp.logical_and(fine, jnp.logical_and(gy + dy >= 0, gy + dy < 8))

    for k, (source, target, dx, dy) in enumerate(moves):
        @pl.when(inside(dx, dy))
        def _(source=source, target=target, dx=dx, dy=dy, k=k):
            halo(source, target, k, dx, dy).start()

    bias = bias_ref[...]

    def conv_row(above, here, below):
        window = jnp.concatenate([above, here, below], axis=1)
        return jnp.dot(window, wmat[...], preferred_element_type=F32)

    def finish(r, total):
        left = pltpu.roll(total[:, 0:C], 1, axis=0)
        right = pltpu.roll(total[:, 2 * C :], COLS - 1, axis=0)
        at = iota((COLS, C), 0)
        left = jnp.where(at == 0, edge[0, pl.ds(r, 1), :], left)
        right = jnp.where(at == COLS - 1, edge[1, pl.ds(r, 1), :], right)
        out = total[:, C : 2 * C] + left + right + bias
        conv_ref[r] = jnp.maximum(out, 0.0).astype(BF16)

    for k, (source, target, dx, dy) in enumerate(moves):
        @pl.when(inside(-dx, -dy))
        def _(source=source, target=target, dx=dx, dy=dy, k=k):
            halo(source, target, k, -dx, -dy).wait_recv()

    for side in range(2):
        ext[0:1, :] = corner_recv[side, 0:8, :].astype(F32)[0:1, :]
        ext[1:17, :] = col_recv[side].astype(F32)
        ext[17:18, :] = corner_recv[2 + side, 0:8, :].astype(F32)[0:1, :]
        window = jnp.concatenate([ext[0:16, :], ext[1:17, :], ext[2:18, :]], axis=1).astype(BF16)
        edge[side] = jnp.dot(
            window, wmat[:, 2 * side * C : (2 * side + 1) * C], preferred_element_type=F32
        )
    finish(0, conv_row(top[...], bev[0], bev[1]))

    def middle(r, carry):
        finish(r, conv_row(bev[r - 1], bev[r], bev[r + 1]))
        return carry

    lax.fori_loop(1, ROWS - 1, middle, 0)
    finish(ROWS - 1, conv_row(bev[ROWS - 2], bev[ROWS - 1], bottom[...]))

    for k, (source, target, dx, dy) in enumerate(moves):
        @pl.when(inside(dx, dy))
        def _(source=source, target=target, dx=dx, dy=dy, k=k):
            halo(source, target, k, dx, dy).wait_send()

    rest = pl.ds(1, DEV - 1)
    pltpu.make_async_copy(send.at[rest], send.at[rest], send_sem).wait()
    pltpu.make_async_copy(cells_in.at[rest], cells_in.at[rest], cell_send_sem).wait()


def shards(point_feats, point_tile, point_cell, point_count, conv_weight, conv_bias):
    vmem = pl.BlockSpec(memory_space=pltpu.VMEM)
    smem = pl.BlockSpec(memory_space=pltpu.SMEM)
    blocks = POINTS // BLOCK
    inv, cells = pl.pallas_call(
        index_kernel,
        name="index",
        out_shape=(
            jax.ShapeDtypeStruct((DEV, 128), jnp.int32),
            jax.ShapeDtypeStruct((DEV, 128), F32),
        ),
        in_specs=[vmem, vmem, smem],
        out_specs=(vmem, vmem),
        scratch_shapes=[pltpu.VMEM((DEV, 128), F32), pltpu.VMEM((DEV, 512), F32)],
    )(point_tile.reshape(blocks, BLOCK), point_cell.reshape(blocks, BLOCK), point_count)
    tile_map = jax.ShapeDtypeStruct((ROWS, COLS, C), BF16)
    dma = pltpu.SemaphoreType.DMA
    return pl.pallas_call(
        main_kernel,
        name="exchange",
        out_shape=(tile_map, tile_map),
        in_specs=[smem, vmem, vmem, vmem, vmem],
        out_specs=(vmem, vmem),
        scratch_shapes=[
            pltpu.VMEM((POINTS + 8, C), F32),
            pltpu.VMEM((CAP, C), F32),
            pltpu.VMEM((DEV, CAP, C), BF16),
            pltpu.VMEM((DEV, CAP, C), BF16),
            pltpu.VMEM((DEV, 1, 128), F32),
            pltpu.VMEM((ROWS // 2, COLS, 2 * C), F32),
            pltpu.VMEM((128, SPAN), BF16),
            pltpu.VMEM((COLS, SPAN), BF16),
            pltpu.VMEM((SPAN, C), BF16),
            pltpu.VMEM((GROUP, 128), F32),
            pltpu.VMEM((3 * C, 3 * C), BF16),
            pltpu.VMEM((ROWS, COLS, C), BF16),
            pltpu.VMEM((COLS, C), BF16),
            pltpu.VMEM((COLS, C), BF16),
            pltpu.VMEM((2, ROWS, C), BF16),
            pltpu.VMEM((2, ROWS, C), BF16),
            pltpu.VMEM((4, 16, C), BF16),
            pltpu.VMEM((4, 16, C), BF16),
            pltpu.VMEM((24, C), F32),
            pltpu.VMEM((2, ROWS, C), F32),
            pltpu.VMEM((2, ROWS, C), F32),
            dma,
            dma,
            dma((GROUPS,)),
            dma((GROUPS,)),
            dma((8,)),
            dma((8,)),
        ],
        compiler_params=pltpu.CompilerParams(
            collective_id=0, has_side_effects=True, vmem_limit_bytes=56 * 1024 * 1024
        ),
    )(inv, point_feats, cells.reshape(DEV, 1, 128), conv_weight, conv_bias.reshape(1, C))


def solution(mesh):
    in_specs = (
        P(("gx", "gy"), None),
        P(("gx", "gy"), None),
        P(("gx", "gy")),
        P(("gx", "gy")),
        P(),
        P(),
    )
    out_specs = (P("gx", "gy", None), P("gx", "gy", None))
    return jax.shard_map(shards, mesh=mesh, in_specs=in_specs, out_specs=out_specs, check_vma=False)
```

```python
import functools

import jax
import jax.numpy as jnp
from jax import lax
from jax.experimental import pallas as pl
from jax.experimental.pallas import tpu as pltpu
from jax.sharding import PartitionSpec as P

MESH = pl.DeviceIdType.MESH
F32 = jnp.float32
BF16 = jnp.bfloat16
C = 128
COLS = 256
ROWS = 16
POINTS = 8192
CAP = 80
DEV = 128
GROUP = 16
GROUPS = DEV // GROUP
SPAN = GROUP * CAP
STRIDE = 27
WIDTH = CAP + 2
BLOCK = 256
CHUNK = 2048


def iota(shape, dim):
    return lax.broadcasted_iota(jnp.int32, shape, dim)


def place():
    gx = lax.axis_index("gx")
    gy = lax.axis_index("gy")
    return lax.rem(gx, 4), lax.div(gx, 4), lax.div(gy, 2), lax.rem(gy, 2)


def partner(i):
    x, y, z, c = place()
    o = lax.rem(i * STRIDE, DEV)
    tc = lax.rem(c + lax.rem(o, 2), 2)
    tz = lax.rem(z + lax.rem(lax.div(o, 2), 4), 4)
    tx = lax.rem(x + lax.rem(lax.div(o, 8), 4), 4)
    ty = lax.rem(y + lax.div(o, 32), 4)
    return ty * 4 + tx, tz * 2 + tc


def main_kernel(
    tile_hbm, cell_hbm, count_ref, feats_hbm, w_hbm, bias_hbm, bev_hbm, conv_hbm,
    bev_ref, conv_ref, tile_ref, cell_ref, w_ref, bias_ref, feats, src, hits, values, table, offs, inv_vmem, inv, row_tab, col_tab,
    stage, send, recv, acc, expand, onehot, row_bc, xs, wmat, top, bottom,
    col_send, col_recv, corner_send, corner_recv, ext, edge, stage_col, edge_pre,
    load_sem, store_sem, inv_sem, send_sem, recv_sem, halo_send_sem, halo_sem,
):
    gx = lax.axis_index("gx")
    gy = lax.axis_index("gy")
    arrays = (
        (tile_hbm, tile_ref), (cell_hbm, cell_ref), (feats_hbm, feats), (w_hbm, w_ref),
        (bias_hbm, bias_ref),
    )
    loads = [pltpu.make_async_copy(a, b, load_sem.at[k]) for k, (a, b) in enumerate(arrays)]
    for load in loads:
        load.start()
    zero_row = jnp.zeros((COLS, C), BF16)
    top[...] = zero_row
    bottom[...] = zero_row
    col_recv[...] = jnp.zeros_like(col_recv)
    corner_recv[...] = jnp.zeros_like(corner_recv)

    barrier = pltpu.get_barrier_semaphore()

    def greet(i, carry):
        other = lax.rem(gx * 8 + gy + i, DEV)
        dest = (lax.div(other, 8), lax.rem(other, 8))
        pl.semaphore_signal(barrier, inc=1, device_id=dest, device_id_type=MESH)
        return carry

    lax.fori_loop(1, DEV, greet, 0)

    offs[...] = jnp.zeros_like(offs)
    table[...] = jnp.zeros_like(table)
    values[...] = jnp.zeros_like(values)
    loads[0].wait()
    loads[1].wait()
    upper = (iota((BLOCK, BLOCK), 0) <= iota((BLOCK, BLOCK), 1)).astype(F32).astype(BF16)
    count = count_ref[0]

    def index_chunk(n, carry):
        base = offs[...]
        for b in range(CHUNK // BLOCK):
            line = n * (CHUNK // 128) + 2 * b
            pair = [tile_ref[pl.ds(line + h, 1), :] for h in range(2)]
            tile = jnp.concatenate(pair, axis=1)
            pair = [cell_ref[pl.ds(line + h, 1), :] for h in range(2)]
            cell = jnp.concatenate(pair, axis=1)
            p = n * CHUNK + b * BLOCK + iota((1, BLOCK), 1)
            tile = jnp.where(p < count, tile, DEV)
            hit = iota((DEV, BLOCK), 0) == tile
            hit16 = hit.astype(F32).astype(BF16)
            span = slice(b * BLOCK, (b + 1) * BLOCK)
            hits[:, span] = hit16
            cum = jnp.dot(hit16, upper, preferred_element_type=F32)
            total = cum + jnp.concatenate([base, base], axis=1)
            rank = jnp.sum(jnp.where(hit, total, 0.0), axis=0, keepdims=True) - 1.0
            base = base + jnp.broadcast_to(cum[:, BLOCK - 1 :], (DEV, 128))
            slot = iota((CAP, BLOCK), 0).astype(F32) == rank
            coded = ((p >> 5) + 1, (p & 31) * 8 + (cell >> 9), (cell & 511) - 256)
            for v, value in enumerate(coded):
                part = jnp.where(slot, value.astype(F32), 0.0).astype(BF16)
                values[v * CAP : (v + 1) * CAP, span] = part
        offs[...] = base
        table[...] += lax.dot_general(
            hits[...], values[...], (((1,), (1,)), ((), ())), preferred_element_type=F32
        )
        return carry

    lax.fori_loop(0, POINTS // CHUNK, index_chunk, 0)
    found = table[...]
    first = found[:, 0:128].astype(jnp.int32)
    second = pltpu.roll(found, 256 - CAP, axis=1)[:, 0:128].astype(jnp.int32)
    third = pltpu.roll(found, 256 - 2 * CAP, axis=1)[:, 0:128].astype(jnp.int32)
    filled = first > 0
    inv_vmem[...] = jnp.where(filled, (first - 1) * 32 + (second >> 3), POINTS)
    inv_copy = pltpu.make_async_copy(inv_vmem, inv, inv_sem)
    inv_copy.start()
    cells = (second & 7) * 512 + third + 256
    row_tab[...] = jnp.where(filled, cells >> 8, -1).astype(F32)
    col_tab[...] = (cells & 255).astype(F32)

    loads[2].wait()

    def widen(b, carry):
        at = pl.multiple_of(b * 512, 512)
        src[pl.ds(at, 512), :] = feats[pl.ds(at, 512), :].astype(F32)
        return carry

    lax.fori_loop(0, POINTS // 512, widen, 0)
    src[pl.ds(POINTS, 8), :] = jnp.zeros((8, C), F32)
    stage[...] = jnp.zeros_like(stage)
    inv_copy.wait()
    pl.semaphore_wait(barrier, DEV - 1)

    def feat_copy(i):
        return pltpu.make_async_remote_copy(
            src_ref=send.at[i],
            dst_ref=recv.at[i],
            send_sem=send_sem,
            recv_sem=recv_sem.at[lax.div(i, GROUP)],
            device_id=partner(i),
            device_id_type=MESH,
        )

    def pack(tile):
        for k in range(CAP):
            at = jnp.minimum(jnp.maximum(inv[tile, k], 0), POINTS)
            stage[k : k + 1, :] = src[pl.ds(at, 1), :]
        stage[CAP : CAP + 1, :] = row_tab[pl.ds(tile, 1), :]
        stage[CAP + 1 : WIDTH, :] = col_tab[pl.ds(tile, 1), :]
        return stage[...].astype(BF16)[0:WIDTH]

    def pack_and_send(i, carry):
        dest = partner(i)
        send[i] = pack(dest[0] * 8 + dest[1])

        @pl.when(i > 1)
        def _():
            feat_copy(i - 1).start()

        return carry

    lax.fori_loop(1, DEV, pack_and_send, 0)
    feat_copy(DEV - 1).start()
    recv[0] = pack(gx * 8 + gy)

    loads[3].wait()
    loads[4].wait()
    for a in range(3):
        for b in range(3):
            wmat[a * C : (a + 1) * C, b * C : (b + 1) * C] = w_ref[a, b]
    acc[...] = jnp.zeros_like(acc)
    lane = iota((1, SPAN), 1).astype(F32)
    owner = jnp.floor((lane + 0.5) * (1.0 / CAP))
    within = lane - owner * CAP
    expand[...] = (iota((128, SPAN), 0).astype(F32) == within).astype(F32).astype(BF16)
    eye = iota((128, 128), 0) == iota((128, 128), 1)
    ones = jnp.ones((128, 128), BF16)
    mine = iota((GROUP, SPAN), 0).astype(F32) == owner

    def scatter(g):
        for j in range(GROUP):
            both = recv[g * GROUP + j, CAP:WIDTH, :].astype(F32)
            xs[j : j + 1, :] = both[0:1]
            xs[GROUP + j : GROUP + j + 1, :] = both[1:2]
        dense = jnp.dot(xs[...].astype(BF16), expand[...], preferred_element_type=F32)
        row_line = jnp.sum(jnp.where(mine, dense[0:GROUP], 0.0), axis=0, keepdims=True)
        col_line = jnp.sum(jnp.where(mine, dense[GROUP:], 0.0), axis=0, keepdims=True)
        onehot[...] = (iota((COLS, SPAN), 0).astype(F32) == col_line).astype(F32).astype(BF16)
        for q in range(SPAN // 128):
            span = slice(q * 128, (q + 1) * 128)
            diag = jnp.where(eye, row_line[:, span], 0.0).astype(BF16)
            row_bc[span, :] = jnp.dot(diag, ones, preferred_element_type=F32).astype(BF16)
        at = pl.ds(pl.multiple_of(g * GROUP, GROUP), GROUP)
        points = recv[at, 0:CAP, :].reshape(SPAN, C)
        rows = row_bc[...]
        none = jnp.zeros((), BF16)
        for pair in range(ROWS // 2):
            even = jnp.where(rows == jnp.asarray(2 * pair, BF16), points, none)
            odd = jnp.where(rows == jnp.asarray(2 * pair + 1, BF16), points, none)
            acc[pair] += jnp.dot(
                onehot[...], jnp.concatenate([even, odd], axis=1), preferred_element_type=F32
            )

    def landed(g, first):
        at = pl.ds(g * GROUP + first, GROUP - first)
        pltpu.make_async_copy(recv.at[at], recv.at[at], recv_sem.at[g]).wait()

    landed(0, 1)
    scatter(0)

    def absorb(g, carry):
        landed(g, 0)
        scatter(g)
        return carry

    lax.fori_loop(1, GROUPS, absorb, 0)

    def settle(r):
        line = acc[r // 2, :, (r % 2) * C : (r % 2 + 1) * C]
        bev_ref[r] = line.astype(BF16)
        stage_col[0, r : r + 1, :] = line[0:1, :]
        stage_col[1, r : r + 1, :] = line[COLS - 1 : COLS, :]

    def halo(source, target, k, dx, dy):
        return pltpu.make_async_remote_copy(
            src_ref=source,
            dst_ref=target,
            send_sem=halo_send_sem.at[k],
            recv_sem=halo_sem.at[k],
            device_id=(gx + dx, gy + dy),
            device_id_type=MESH,
        )

    moves = [
        (bev_ref.at[0], bottom, -1, 0),
        (bev_ref.at[ROWS - 1], top, 1, 0),
        (col_send.at[0], col_recv.at[1], 0, -1),
        (col_send.at[1], col_recv.at[0], 0, 1),
        (corner_send.at[0], corner_recv.at[3], -1, -1),
        (corner_send.at[1], corner_recv.at[2], -1, 1),
        (corner_send.at[2], corner_recv.at[1], 1, -1),
        (corner_send.at[3], corner_recv.at[0], 1, 1),
    ]

    def inside(dx, dy):
        fine = jnp.logical_and(gx + dx >= 0, gx + dx < 16)
        return jnp.logical_and(fine, jnp.logical_and(gy + dy >= 0, gy + dy < 8))

    def launch(which):
        for k in which:
            source, target, dx, dy = moves[k]

            @pl.when(inside(dx, dy))
            def _(source=source, target=target, dx=dx, dy=dy, k=k):
                halo(source, target, k, dx, dy).start()

    settle(0)
    settle(ROWS - 1)
    for k in range(4):
        at = (ROWS - 1) * (k // 2)
        corner_send[k] = jnp.broadcast_to(stage_col[k % 2, at : at + 1, :], (16, C)).astype(BF16)
    for r in range(1, ROWS - 1):
        settle(r)
        if r == 2:
            launch((0, 1))
        if r == 6:
            launch((4, 5, 6, 7))
    col_send[0] = stage_col[0].astype(BF16)
    col_send[1] = stage_col[1].astype(BF16)
    bias = bias_ref[...]
    at = iota((COLS, C), 0)

    def finish(r, total):
        left = jnp.where(at == 0, 0.0, pltpu.roll(total[:, 0:C], 1, axis=0))
        right = jnp.where(at == COLS - 1, 0.0, pltpu.roll(total[:, 2 * C :], COLS - 1, axis=0))
        out = total[:, C : 2 * C] + left + right + bias
        edge_pre[0, r] = out[0:16]
        edge_pre[1, r] = out[COLS - 16 :]
        conv_ref[r] = jnp.maximum(out, 0.0).astype(BF16)

    launch((2, 3))
    bev_store = pltpu.make_async_copy(bev_ref, bev_hbm, store_sem.at[0])
    bev_store.start()

    def middle(m, carry):
        r = 2 * m + 1
        rows = [bev_ref[r - 1 + q] for q in range(4)]
        window = jnp.concatenate(
            [jnp.concatenate(rows[q : q + 2], axis=0) for q in range(3)], axis=1
        )
        total = jnp.dot(window, wmat[...], preferred_element_type=F32)
        finish(r, total[0:COLS])
        finish(r + 1, total[COLS:])
        return carry

    lax.fori_loop(0, ROWS // 2 - 1, middle, 0)

    for k, (source, target, dx, dy) in enumerate(moves):
        @pl.when(inside(-dx, -dy))
        def _(source=source, target=target, dx=dx, dy=dy, k=k):
            halo(source, target, k, -dx, -dy).wait_recv()

    window = jnp.concatenate(
        [
            jnp.concatenate([top[...], bev_ref[ROWS - 2]], axis=0),
            jnp.concatenate([bev_ref[0], bev_ref[ROWS - 1]], axis=0),
            jnp.concatenate([bev_ref[1], bottom[...]], axis=0),
        ],
        axis=1,
    )
    total = jnp.dot(window, wmat[...], preferred_element_type=F32)
    finish(0, total[0:COLS])
    finish(ROWS - 1, total[COLS:])
    for side in range(2):
        ext[0:1, :] = corner_recv[side].astype(F32)[0:1, :]
        ext[1:17, :] = col_recv[side].astype(F32)
        ext[17:18, :] = corner_recv[2 + side].astype(F32)[0:1, :]
        window = jnp.concatenate([ext[0:16, :], ext[1:17, :], ext[2:18, :]], axis=1).astype(BF16)
        edge[side] = jnp.dot(
            window, wmat[:, 2 * side * C : (2 * side + 1) * C], preferred_element_type=F32
        )
    small = iota((16, C), 0)
    for r in range(ROWS):
        left = edge_pre[0, r] + jnp.where(small == 0, edge[0, r : r + 1, :], 0.0)
        conv_ref[r, 0:16, :] = jnp.maximum(left, 0.0).astype(BF16)
        right = edge_pre[1, r] + jnp.where(small == 15, edge[1, r : r + 1, :], 0.0)
        conv_ref[r, COLS - 16 :, :] = jnp.maximum(right, 0.0).astype(BF16)

    conv_store = pltpu.make_async_copy(conv_ref, conv_hbm, store_sem.at[1])
    conv_store.start()
    for k, (source, target, dx, dy) in enumerate(moves):
        @pl.when(inside(dx, dy))
        def _(source=source, target=target, dx=dx, dy=dy, k=k):
            halo(source, target, k, dx, dy).wait_send()

    rest = pl.ds(1, DEV - 1)
    pltpu.make_async_copy(send.at[rest], send.at[rest], send_sem).wait()
    bev_store.wait()
    conv_store.wait()


def shards(point_feats, point_tile, point_cell, point_count, conv_weight, conv_bias):
    smem = pl.BlockSpec(memory_space=pltpu.SMEM)
    hbm = pl.BlockSpec(memory_space=pltpu.HBM)
    tile_map = jax.ShapeDtypeStruct((ROWS, COLS, C), BF16)
    dma = pltpu.SemaphoreType.DMA
    return pl.pallas_call(
        main_kernel,
        name="exchange",
        out_shape=(tile_map, tile_map),
        in_specs=[hbm, hbm, smem, hbm, hbm, hbm],
        out_specs=(hbm, hbm),
        scratch_shapes=[
            pltpu.VMEM((ROWS, COLS, C), BF16),
            pltpu.VMEM((ROWS, COLS, C), BF16),
            pltpu.VMEM((POINTS // 128, 128), jnp.int32),
            pltpu.VMEM((POINTS // 128, 128), jnp.int32),
            pltpu.VMEM((3, 3, C, C), BF16),
            pltpu.VMEM((1, C), F32),
            pltpu.VMEM((POINTS, C), BF16),
            pltpu.VMEM((POINTS + 8, C), F32),
            pltpu.VMEM((DEV, CHUNK), BF16),
            pltpu.VMEM((256, CHUNK), BF16),
            pltpu.VMEM((DEV, 256), F32),
            pltpu.VMEM((DEV, 128), F32),
            pltpu.VMEM((DEV, 128), jnp.int32),
            pltpu.SMEM((DEV, 128), jnp.int32),
            pltpu.VMEM((DEV, 128), F32),
            pltpu.VMEM((DEV, 128), F32),
            pltpu.VMEM((96, C), F32),
            pltpu.VMEM((DEV, WIDTH, C), BF16),
            pltpu.VMEM((DEV, WIDTH, C), BF16),
            pltpu.VMEM((ROWS // 2, COLS, 2 * C), F32),
            pltpu.VMEM((128, SPAN), BF16),
            pltpu.VMEM((COLS, SPAN), BF16),
            pltpu.VMEM((SPAN, C), BF16),
            pltpu.VMEM((2 * GROUP, 128), F32),
            pltpu.VMEM((3 * C, 3 * C), BF16),
            pltpu.VMEM((COLS, C), BF16),
            pltpu.VMEM((COLS, C), BF16),
            pltpu.VMEM((2, ROWS, C), BF16),
            pltpu.VMEM((2, ROWS, C), BF16),
            pltpu.VMEM((4, 16, C), BF16),
            pltpu.VMEM((4, 16, C), BF16),
            pltpu.VMEM((24, C), F32),
            pltpu.VMEM((2, ROWS, C), F32),
            pltpu.VMEM((2, ROWS, C), F32),
            pltpu.VMEM((2, ROWS, 16, C), F32),
            dma((5,)),
            dma((2,)),
            dma,
            dma,
            dma((GROUPS,)),
            dma((8,)),
            dma((8,)),
        ],
        compiler_params=pltpu.CompilerParams(
            collective_id=0, has_side_effects=True, vmem_limit_bytes=63 * 1024 * 1024
        ),
    )(
        point_tile.reshape(POINTS // 128, 128),
        point_cell.reshape(POINTS // 128, 128),
        point_count,
        point_feats,
        conv_weight,
        conv_bias.reshape(1, C),
    )


def solution(mesh):
    in_specs = (
        P(("gx", "gy"), None),
        P(("gx", "gy"), None),
        P(("gx", "gy")),
        P(("gx", "gy")),
        P(),
        P(),
    )
    out_specs = (P("gx", "gy", None), P("gx", "gy", None))
    return jax.shard_map(shards, mesh=mesh, in_specs=in_specs, out_specs=out_specs, check_vma=False)
```

```python
import functools

import jax
import jax.numpy as jnp
from jax import lax
from jax.experimental import pallas as pl
from jax.experimental.pallas import tpu as pltpu
from jax.sharding import PartitionSpec as P

MESH = pl.DeviceIdType.MESH
F32 = jnp.float32
BF16 = jnp.bfloat16
C = 128
COLS = 256
ROWS = 16
POINTS = 8192
CAP = 80
DEV = 128
GROUP = 16
GROUPS = DEV // GROUP
SPAN = GROUP * CAP
STRIDE = 27
LAG = 4
WIDTH = CAP + 2
BLOCK = 256
CHUNK = 2048


def iota(shape, dim):
    return lax.broadcasted_iota(jnp.int32, shape, dim)


def place():
    gx = lax.axis_index("gx")
    gy = lax.axis_index("gy")
    return lax.rem(gx, 4), lax.div(gx, 4), lax.div(gy, 2), lax.rem(gy, 2)


def partner(i):
    x, y, z, c = place()
    o = lax.rem(i * STRIDE, DEV)
    tc = lax.rem(c + lax.rem(o, 2), 2)
    tz = lax.rem(z + lax.rem(lax.div(o, 2), 4), 4)
    tx = lax.rem(x + lax.rem(lax.div(o, 8), 4), 4)
    ty = lax.rem(y + lax.div(o, 32), 4)
    return ty * 4 + tx, tz * 2 + tc


def main_kernel(
    tile_hbm, cell_hbm, count_ref, feats_hbm, w_hbm, bias_hbm, bev_ref, conv_ref,
    tile_ref, cell_ref, w_ref, bias_ref, feats, src, hits, values, table, offs, inv_vmem, inv, row_tab, col_tab,
    stage, send, recv, acc, expand, onehot, row_bc, xs, wmat, top, bottom,
    col_send, col_recv, corner_send, corner_recv, ext, edge, stage_col, edge_pre,
    load_sem, inv_sem, send_sem, recv_sem, halo_send_sem, halo_sem,
):
    gx = lax.axis_index("gx")
    gy = lax.axis_index("gy")
    arrays = (
        (tile_hbm, tile_ref), (cell_hbm, cell_ref), (feats_hbm, feats), (w_hbm, w_ref),
        (bias_hbm, bias_ref),
    )
    loads = [pltpu.make_async_copy(a, b, load_sem.at[k]) for k, (a, b) in enumerate(arrays)]
    for load in loads:
        load.start()
    zero_row = jnp.zeros((COLS, C), BF16)
    top[...] = zero_row
    bottom[...] = zero_row
    col_recv[...] = jnp.zeros_like(col_recv)
    corner_recv[...] = jnp.zeros_like(corner_recv)

    barrier = pltpu.get_barrier_semaphore()

    def greet(i, carry):
        other = lax.rem(gx * 8 + gy + i, DEV)
        dest = (lax.div(other, 8), lax.rem(other, 8))
        pl.semaphore_signal(barrier, inc=1, device_id=dest, device_id_type=MESH)
        return carry

    lax.fori_loop(1, DEV, greet, 0)

    offs[...] = jnp.zeros_like(offs)
    table[...] = jnp.zeros_like(table)
    values[...] = jnp.zeros_like(values)
    loads[0].wait()
    loads[1].wait()
    upper = (iota((BLOCK, BLOCK), 0) <= iota((BLOCK, BLOCK), 1)).astype(F32).astype(BF16)
    count = count_ref[0]

    loads[2].wait()

    def index_chunk(n, carry):
        base = offs[...]
        at = pl.multiple_of(n * CHUNK, CHUNK)
        src[pl.ds(at, CHUNK), :] = feats[pl.ds(at, CHUNK), :].astype(F32)
        for b in range(CHUNK // BLOCK):
            line = n * (CHUNK // 128) + 2 * b
            pair = [tile_ref[pl.ds(line + h, 1), :] for h in range(2)]
            tile = jnp.concatenate(pair, axis=1)
            pair = [cell_ref[pl.ds(line + h, 1), :] for h in range(2)]
            cell = jnp.concatenate(pair, axis=1)
            p = n * CHUNK + b * BLOCK + iota((1, BLOCK), 1)
            tile = jnp.where(p < count, tile, DEV)
            hit = iota((DEV, BLOCK), 0) == tile
            hit16 = hit.astype(F32).astype(BF16)
            span = slice(b * BLOCK, (b + 1) * BLOCK)
            hits[:, span] = hit16
            cum = jnp.dot(hit16, upper, preferred_element_type=F32)
            total = cum + jnp.concatenate([base, base], axis=1)
            rank = jnp.sum(jnp.where(hit, total, 0.0), axis=0, keepdims=True) - 1.0
            base = base + jnp.broadcast_to(cum[:, BLOCK - 1 :], (DEV, 128))
            slot = iota((CAP, BLOCK), 0).astype(F32) == rank
            coded = ((p >> 5) + 1, (p & 31) * 8 + (cell >> 9), (cell & 511) - 256)
            for v, value in enumerate(coded):
                part = jnp.where(slot, value.astype(F32), 0.0).astype(BF16)
                values[v * CAP : (v + 1) * CAP, span] = part
        offs[...] = base
        table[...] += lax.dot_general(
            hits[...], values[...], (((1,), (1,)), ((), ())), preferred_element_type=F32
        )
        return carry

    lax.fori_loop(0, POINTS // CHUNK, index_chunk, 0)
    found = table[...]
    first = found[:, 0:128].astype(jnp.int32)
    second = pltpu.roll(found, 256 - CAP, axis=1)[:, 0:128].astype(jnp.int32)
    third = pltpu.roll(found, 256 - 2 * CAP, axis=1)[:, 0:128].astype(jnp.int32)
    filled = first > 0
    inv_vmem[...] = jnp.where(filled, (first - 1) * 32 + (second >> 3), POINTS)
    inv_copy = pltpu.make_async_copy(inv_vmem, inv, inv_sem)
    inv_copy.start()
    cells = (second & 7) * 512 + third + 256
    row_tab[...] = jnp.where(filled, cells >> 8, -1).astype(F32)
    col_tab[...] = (cells & 255).astype(F32)


    src[pl.ds(POINTS, 8), :] = jnp.zeros((8, C), F32)
    stage[...] = jnp.zeros_like(stage)
    inv_copy.wait()
    pl.semaphore_wait(barrier, DEV - 1)

    def feat_copy(i):
        return pltpu.make_async_remote_copy(
            src_ref=send.at[i],
            dst_ref=recv.at[i],
            send_sem=send_sem,
            recv_sem=recv_sem.at[lax.div(i, GROUP)],
            device_id=partner(i),
            device_id_type=MESH,
        )

    def pack(tile):
        for k in range(CAP):
            at = jnp.minimum(jnp.maximum(inv[tile, k], 0), POINTS)
            stage[k : k + 1, :] = src[pl.ds(at, 1), :]
        stage[CAP : CAP + 1, :] = row_tab[pl.ds(tile, 1), :]
        stage[CAP + 1 : WIDTH, :] = col_tab[pl.ds(tile, 1), :]
        return stage[...].astype(BF16)[0:WIDTH]

    loads[3].wait()
    loads[4].wait()
    for a in range(3):
        for b in range(3):
            wmat[a * C : (a + 1) * C, b * C : (b + 1) * C] = w_ref[a, b]
    acc[...] = jnp.zeros_like(acc)
    lane = iota((1, SPAN), 1).astype(F32)
    owner = jnp.floor((lane + 0.5) * (1.0 / CAP))
    within = lane - owner * CAP
    expand[...] = (iota((128, SPAN), 0).astype(F32) == within).astype(F32).astype(BF16)
    eye = iota((128, 128), 0) == iota((128, 128), 1)
    ones = jnp.ones((128, 128), BF16)
    mine = iota((GROUP, SPAN), 0).astype(F32) == owner

    def scatter(g):
        for j in range(GROUP):
            both = recv[g * GROUP + j, CAP:WIDTH, :].astype(F32)
            xs[j : j + 1, :] = both[0:1]
            xs[GROUP + j : GROUP + j + 1, :] = both[1:2]
        dense = jnp.dot(xs[...].astype(BF16), expand[...], preferred_element_type=F32)
        row_line = jnp.sum(jnp.where(mine, dense[0:GROUP], 0.0), axis=0, keepdims=True)
        col_line = jnp.sum(jnp.where(mine, dense[GROUP:], 0.0), axis=0, keepdims=True)
        onehot[...] = (iota((COLS, SPAN), 0).astype(F32) == col_line).astype(F32).astype(BF16)
        for q in range(SPAN // 128):
            span = slice(q * 128, (q + 1) * 128)
            diag = jnp.where(eye, row_line[:, span], 0.0).astype(BF16)
            row_bc[span, :] = jnp.dot(diag, ones, preferred_element_type=F32).astype(BF16)
        at = pl.ds(pl.multiple_of(g * GROUP, GROUP), GROUP)
        points = recv[at, 0:CAP, :].reshape(SPAN, C)
        rows = row_bc[...]
        none = jnp.zeros((), BF16)
        for pair in range(ROWS // 2):
            even = jnp.where(rows == jnp.asarray(2 * pair, BF16), points, none)
            odd = jnp.where(rows == jnp.asarray(2 * pair + 1, BF16), points, none)
            acc[pair] += jnp.dot(
                onehot[...], jnp.concatenate([even, odd], axis=1), preferred_element_type=F32
            )

    def landed(g, first):
        at = pl.ds(g * GROUP + first, GROUP - first)
        pltpu.make_async_copy(recv.at[at], recv.at[at], recv_sem.at[g]).wait()

    recv[0] = pack(gx * 8 + gy)

    def absorb(g, carry):
        @pl.when(g == 0)
        def _():
            landed(0, 1)

        @pl.when(g > 0)
        def _():
            landed(g, 0)

        scatter(g)
        return carry

    def batch(g, carry):
        first = jnp.maximum(g * GROUP, 1)
        end = (g + 1) * GROUP

        def pack_and_send(i, carry):
            dest = partner(i)
            send[i] = pack(dest[0] * 8 + dest[1])

            @pl.when(i > first)
            def _():
                feat_copy(i - 1).start()

            return carry

        lax.fori_loop(first, end, pack_and_send, 0)
        feat_copy(end - 1).start()

        @pl.when(g >= LAG)
        def _():
            absorb(g - LAG, 0)

        return carry

    lax.fori_loop(0, GROUPS, batch, 0)
    lax.fori_loop(GROUPS - LAG, GROUPS, absorb, 0)

    def settle(r):
        line = acc[r // 2, :, (r % 2) * C : (r % 2 + 1) * C]
        bev_ref[r] = line.astype(BF16)
        stage_col[0, r : r + 1, :] = line[0:1, :]
        stage_col[1, r : r + 1, :] = line[COLS - 1 : COLS, :]

    def halo(source, target, k, dx, dy):
        return pltpu.make_async_remote_copy(
            src_ref=source,
            dst_ref=target,
            send_sem=halo_send_sem.at[k],
            recv_sem=halo_sem.at[k],
            device_id=(gx + dx, gy + dy),
            device_id_type=MESH,
        )

    moves = [
        (bev_ref.at[0], bottom, -1, 0),
        (bev_ref.at[ROWS - 1], top, 1, 0),
        (col_send.at[0], col_recv.at[1], 0, -1),
        (col_send.at[1], col_recv.at[0], 0, 1),
        (corner_send.at[0], corner_recv.at[3], -1, -1),
        (corner_send.at[1], corner_recv.at[2], -1, 1),
        (corner_send.at[2], corner_recv.at[1], 1, -1),
        (corner_send.at[3], corner_recv.at[0], 1, 1),
    ]

    def inside(dx, dy):
        fine = jnp.logical_and(gx + dx >= 0, gx + dx < 16)
        return jnp.logical_and(fine, jnp.logical_and(gy + dy >= 0, gy + dy < 8))

    def launch(which):
        for k in which:
            source, target, dx, dy = moves[k]

            @pl.when(inside(dx, dy))
            def _(source=source, target=target, dx=dx, dy=dy, k=k):
                halo(source, target, k, dx, dy).start()

    settle(0)
    settle(ROWS - 1)
    for k in range(4):
        at = (ROWS - 1) * (k // 2)
        corner_send[k] = jnp.broadcast_to(stage_col[k % 2, at : at + 1, :], (16, C)).astype(BF16)
    for r in range(1, ROWS - 1):
        settle(r)
        if r == 2:
            launch((0, 1))
        if r == 6:
            launch((4, 5, 6, 7))
    col_send[0] = stage_col[0].astype(BF16)
    col_send[1] = stage_col[1].astype(BF16)
    bias = bias_ref[...]
    at = iota((COLS, C), 0)

    def finish(r, total):
        left = jnp.where(at == 0, 0.0, pltpu.roll(total[:, 0:C], 1, axis=0))
        right = jnp.where(at == COLS - 1, 0.0, pltpu.roll(total[:, 2 * C :], COLS - 1, axis=0))
        out = total[:, C : 2 * C] + left + right + bias
        edge_pre[0, r] = out[0:16]
        edge_pre[1, r] = out[COLS - 16 :]
        conv_ref[r] = jnp.maximum(out, 0.0).astype(BF16)

    launch((2, 3))

    def middle(m, carry):
        r = 2 * m + 1
        rows = [bev_ref[r - 1 + q] for q in range(4)]
        window = jnp.concatenate(
            [jnp.concatenate(rows[q : q + 2], axis=0) for q in range(3)], axis=1
        )
        total = jnp.dot(window, wmat[...], preferred_element_type=F32)
        finish(r, total[0:COLS])
        finish(r + 1, total[COLS:])
        return carry

    lax.fori_loop(0, ROWS // 2 - 1, middle, 0)

    for k, (source, target, dx, dy) in enumerate(moves):
        @pl.when(inside(-dx, -dy))
        def _(source=source, target=target, dx=dx, dy=dy, k=k):
            halo(source, target, k, -dx, -dy).wait_recv()

    window = jnp.concatenate(
        [
            jnp.concatenate([top[...], bev_ref[ROWS - 2]], axis=0),
            jnp.concatenate([bev_ref[0], bev_ref[ROWS - 1]], axis=0),
            jnp.concatenate([bev_ref[1], bottom[...]], axis=0),
        ],
        axis=1,
    )
    total = jnp.dot(window, wmat[...], preferred_element_type=F32)
    finish(0, total[0:COLS])
    finish(ROWS - 1, total[COLS:])
    for side in range(2):
        ext[0:1, :] = corner_recv[side].astype(F32)[0:1, :]
        ext[1:17, :] = col_recv[side].astype(F32)
        ext[17:18, :] = corner_recv[2 + side].astype(F32)[0:1, :]
        window = jnp.concatenate([ext[0:16, :], ext[1:17, :], ext[2:18, :]], axis=1).astype(BF16)
        edge[side] = jnp.dot(
            window, wmat[:, 2 * side * C : (2 * side + 1) * C], preferred_element_type=F32
        )
    small = iota((16, C), 0)
    for r in range(ROWS):
        left = edge_pre[0, r] + jnp.where(small == 0, edge[0, r : r + 1, :], 0.0)
        conv_ref[r, 0:16, :] = jnp.maximum(left, 0.0).astype(BF16)
        right = edge_pre[1, r] + jnp.where(small == 15, edge[1, r : r + 1, :], 0.0)
        conv_ref[r, COLS - 16 :, :] = jnp.maximum(right, 0.0).astype(BF16)

    for k, (source, target, dx, dy) in enumerate(moves):
        @pl.when(inside(dx, dy))
        def _(source=source, target=target, dx=dx, dy=dy, k=k):
            halo(source, target, k, dx, dy).wait_send()

    rest = pl.ds(1, DEV - 1)
    pltpu.make_async_copy(send.at[rest], send.at[rest], send_sem).wait()


def shards(point_feats, point_tile, point_cell, point_count, conv_weight, conv_bias):
    smem = pl.BlockSpec(memory_space=pltpu.SMEM)
    vmem = pl.BlockSpec(memory_space=pltpu.VMEM)
    hbm = pl.BlockSpec(memory_space=pltpu.HBM)
    tile_map = pltpu.VMEM((ROWS, COLS, C), BF16)
    dma = pltpu.SemaphoreType.DMA
    return pl.pallas_call(
        main_kernel,
        name="exchange",
        out_shape=(tile_map, tile_map),
        in_specs=[hbm, hbm, smem, hbm, hbm, hbm],
        out_specs=(vmem, vmem),
        scratch_shapes=[
            pltpu.VMEM((POINTS // 128, 128), jnp.int32),
            pltpu.VMEM((POINTS // 128, 128), jnp.int32),
            pltpu.VMEM((3, 3, C, C), BF16),
            pltpu.VMEM((1, C), F32),
            pltpu.VMEM((POINTS, C), BF16),
            pltpu.VMEM((POINTS + 8, C), F32),
            pltpu.VMEM((DEV, CHUNK), BF16),
            pltpu.VMEM((256, CHUNK), BF16),
            pltpu.VMEM((DEV, 256), F32),
            pltpu.VMEM((DEV, 128), F32),
            pltpu.VMEM((DEV, 128), jnp.int32),
            pltpu.SMEM((DEV, 128), jnp.int32),
            pltpu.VMEM((DEV, 128), F32),
            pltpu.VMEM((DEV, 128), F32),
            pltpu.VMEM((96, C), F32),
            pltpu.VMEM((DEV, WIDTH, C), BF16),
            pltpu.VMEM((DEV, WIDTH, C), BF16),
            pltpu.VMEM((ROWS // 2, COLS, 2 * C), F32),
            pltpu.VMEM((128, SPAN), BF16),
            pltpu.VMEM((COLS, SPAN), BF16),
            pltpu.VMEM((SPAN, C), BF16),
            pltpu.VMEM((2 * GROUP, 128), F32),
            pltpu.VMEM((3 * C, 3 * C), BF16),
            pltpu.VMEM((COLS, C), BF16),
            pltpu.VMEM((COLS, C), BF16),
            pltpu.VMEM((2, ROWS, C), BF16),
            pltpu.VMEM((2, ROWS, C), BF16),
            pltpu.VMEM((4, 16, C), BF16),
            pltpu.VMEM((4, 16, C), BF16),
            pltpu.VMEM((24, C), F32),
            pltpu.VMEM((2, ROWS, C), F32),
            pltpu.VMEM((2, ROWS, C), F32),
            pltpu.VMEM((2, ROWS, 16, C), F32),
            dma((5,)),
            dma,
            dma,
            dma((GROUPS,)),
            dma((8,)),
            dma((8,)),
        ],
        compiler_params=pltpu.CompilerParams(
            collective_id=0, has_side_effects=True, vmem_limit_bytes=64929792
        ),
    )(
        point_tile.reshape(POINTS // 128, 128),
        point_cell.reshape(POINTS // 128, 128),
        point_count,
        point_feats,
        conv_weight,
        conv_bias.reshape(1, C),
    )


def solution(mesh):
    in_specs = (
        P(("gx", "gy"), None),
        P(("gx", "gy"), None),
        P(("gx", "gy")),
        P(("gx", "gy")),
        P(),
        P(),
    )
    out_specs = (P("gx", "gy", None), P("gx", "gy", None))
    return jax.shard_map(shards, mesh=mesh, in_specs=in_specs, out_specs=out_specs, check_vma=False)
```

```python
import functools

import jax
import jax.numpy as jnp
from jax import lax
from jax.experimental import pallas as pl
from jax.experimental.pallas import tpu as pltpu
from jax.sharding import PartitionSpec as P

MESH = pl.DeviceIdType.MESH
F32 = jnp.float32
BF16 = jnp.bfloat16
C = 128
COLS = 256
ROWS = 16
POINTS = 8192
CAP = 80
DEV = 128
GROUP = 16
GROUPS = DEV // GROUP
SPAN = GROUP * CAP
STRIDE = 27
LAG = 4
BLOCK = 256
CHUNK = 2048


def iota(shape, dim):
    return lax.broadcasted_iota(jnp.int32, shape, dim)


def place():
    gx = lax.axis_index("gx")
    gy = lax.axis_index("gy")
    return lax.rem(gx, 4), lax.div(gx, 4), lax.div(gy, 2), lax.rem(gy, 2)


def partner(i):
    x, y, z, c = place()
    o = lax.rem(i * STRIDE, DEV)
    tc = lax.rem(c + lax.rem(o, 2), 2)
    tz = lax.rem(z + lax.rem(lax.div(o, 2), 4), 4)
    tx = lax.rem(x + lax.rem(lax.div(o, 8), 4), 4)
    ty = lax.rem(y + lax.div(o, 32), 4)
    return ty * 4 + tx, tz * 2 + tc


def main_kernel(
    tile_hbm, cell_hbm, count_ref, feats_hbm, w_hbm, bias_hbm, bev_ref, conv_ref,
    tile_ref, cell_ref, w_ref, bias_ref, feats, src, hits, values, table, offs, inv_vmem, inv, cell_tab, cell_send, cells_in,
    stage, send, recv, acc, expand, onehot, row_bc, xs, wmat, top, bottom,
    col_send, col_recv, corner_send, corner_recv, ext, edge, stage_col, edge_pre,
    load_sem, inv_sem, send_sem, recv_sem, cell_send_sem, cell_sem, halo_send_sem, halo_sem,
):
    gx = lax.axis_index("gx")
    gy = lax.axis_index("gy")
    arrays = (
        (tile_hbm, tile_ref), (cell_hbm, cell_ref), (feats_hbm, feats), (w_hbm, w_ref),
        (bias_hbm, bias_ref),
    )
    loads = [pltpu.make_async_copy(a, b, load_sem.at[k]) for k, (a, b) in enumerate(arrays)]
    for load in loads:
        load.start()
    zero_row = jnp.zeros((COLS, C), BF16)
    top[...] = zero_row
    bottom[...] = zero_row
    col_recv[...] = jnp.zeros_like(col_recv)
    corner_recv[...] = jnp.zeros_like(corner_recv)

    barrier = pltpu.get_barrier_semaphore()

    def greet(i, carry):
        other = lax.rem(gx * 8 + gy + i, DEV)
        dest = (lax.div(other, 8), lax.rem(other, 8))
        pl.semaphore_signal(barrier, inc=1, device_id=dest, device_id_type=MESH)
        return carry

    lax.fori_loop(1, DEV, greet, 0)

    offs[...] = jnp.zeros_like(offs)
    table[...] = jnp.zeros_like(table)
    values[...] = jnp.zeros_like(values)
    loads[0].wait()
    loads[1].wait()
    upper = (iota((BLOCK, BLOCK), 0) <= iota((BLOCK, BLOCK), 1)).astype(F32).astype(BF16)
    count = count_ref[0]

    loads[2].wait()

    def index_chunk(n, carry):
        base = offs[...]
        at = pl.multiple_of(n * CHUNK, CHUNK)
        src[pl.ds(at, CHUNK), :] = feats[pl.ds(at, CHUNK), :].astype(F32)
        for b in range(CHUNK // BLOCK):
            line = n * (CHUNK // 128) + 2 * b
            pair = [tile_ref[pl.ds(line + h, 1), :] for h in range(2)]
            tile = jnp.concatenate(pair, axis=1)
            pair = [cell_ref[pl.ds(line + h, 1), :] for h in range(2)]
            cell = jnp.concatenate(pair, axis=1)
            p = n * CHUNK + b * BLOCK + iota((1, BLOCK), 1)
            tile = jnp.where(p < count, tile, DEV)
            hit = iota((DEV, BLOCK), 0) == tile
            hit16 = hit.astype(F32).astype(BF16)
            span = slice(b * BLOCK, (b + 1) * BLOCK)
            hits[:, span] = hit16
            cum = jnp.dot(hit16, upper, preferred_element_type=F32)
            total = cum + jnp.concatenate([base, base], axis=1)
            rank = jnp.sum(jnp.where(hit, total, 0.0), axis=0, keepdims=True) - 1.0
            base = base + jnp.broadcast_to(cum[:, BLOCK - 1 :], (DEV, 128))
            slot = iota((CAP, BLOCK), 0).astype(F32) == rank
            coded = ((p >> 5) + 1, (p & 31) * 8 + (cell >> 9), (cell & 511) - 256)
            for v, value in enumerate(coded):
                part = jnp.where(slot, value.astype(F32), 0.0).astype(BF16)
                values[v * CAP : (v + 1) * CAP, span] = part
        offs[...] = base
        table[...] += lax.dot_general(
            hits[...], values[...], (((1,), (1,)), ((), ())), preferred_element_type=F32
        )
        return carry

    lax.fori_loop(0, POINTS // CHUNK, index_chunk, 0)
    found = table[...]
    first = found[:, 0:128].astype(jnp.int32)
    second = pltpu.roll(found, 256 - CAP, axis=1)[:, 0:128].astype(jnp.int32)
    third = pltpu.roll(found, 256 - 2 * CAP, axis=1)[:, 0:128].astype(jnp.int32)
    filled = first > 0
    inv_vmem[...] = jnp.where(filled, (first - 1) * 32 + (second >> 3), POINTS)
    inv_copy = pltpu.make_async_copy(inv_vmem, inv, inv_sem)
    inv_copy.start()
    cells = (second & 7) * 512 + third + 256
    cell_tab[...] = jnp.where(filled, cells, -1).astype(F32)


    src[pl.ds(POINTS, 8), :] = jnp.zeros((8, C), F32)
    inv_copy.wait()
    pl.semaphore_wait(barrier, DEV - 1)

    def cell_copy(i, dest):
        return pltpu.make_async_remote_copy(
            src_ref=cell_send.at[i],
            dst_ref=cells_in.at[i],
            send_sem=cell_send_sem,
            recv_sem=cell_sem.at[lax.div(i, GROUP)],
            device_id=dest,
            device_id_type=MESH,
        )

    def feat_copy(i, dest):
        return pltpu.make_async_remote_copy(
            src_ref=send.at[i],
            dst_ref=recv.at[i],
            send_sem=send_sem,
            recv_sem=recv_sem.at[lax.div(i, GROUP)],
            device_id=dest,
            device_id_type=MESH,
        )

    def ship(i):
        dest = partner(i)
        cell_copy(i, dest).start()
        feat_copy(i, dest).start()

    def pack(tile):
        for k in range(CAP):
            at = jnp.minimum(jnp.maximum(inv[tile, k], 0), POINTS)
            stage[k : k + 1, :] = src[pl.ds(at, 1), :]
        return stage[...].astype(BF16)

    lane = iota((1, SPAN), 1).astype(F32)
    owner = jnp.floor((lane + 0.5) * (1.0 / CAP))
    within = lane - owner * CAP
    eye = iota((128, 128), 0) == iota((128, 128), 1)
    ones = jnp.ones((128, 128), BF16)
    mine = iota((GROUP, SPAN), 0).astype(F32) == owner

    def scatter(g):
        for j in range(GROUP):
            xs[j : j + 1, :] = cells_in[g * GROUP + j]
        cell = xs[...]
        row = jnp.floor(cell * (1.0 / COLS))
        both = jnp.concatenate([row, cell - row * COLS], axis=0).astype(BF16)
        dense = jnp.dot(both, expand[...], preferred_element_type=F32)
        row_line = jnp.sum(jnp.where(mine, dense[0:GROUP], 0.0), axis=0, keepdims=True)
        col_line = jnp.sum(jnp.where(mine, dense[GROUP:], 0.0), axis=0, keepdims=True)
        onehot[...] = (iota((COLS, SPAN), 0).astype(F32) == col_line).astype(F32).astype(BF16)
        for q in range(SPAN // 128):
            span = slice(q * 128, (q + 1) * 128)
            diag = jnp.where(eye, row_line[:, span], 0.0).astype(BF16)
            row_bc[span, :] = jnp.dot(diag, ones, preferred_element_type=F32).astype(BF16)
        at = pl.ds(pl.multiple_of(g * GROUP, GROUP), GROUP)
        points = recv[at].reshape(SPAN, C)
        rows = row_bc[...]
        none = jnp.zeros((), BF16)
        for pair in range(ROWS // 2):
            even = jnp.where(rows == jnp.asarray(2 * pair, BF16), points, none)
            odd = jnp.where(rows == jnp.asarray(2 * pair + 1, BF16), points, none)
            acc[pair] += jnp.dot(
                onehot[...], jnp.concatenate([even, odd], axis=1), preferred_element_type=F32
            )

    def landed(g, first):
        at = pl.ds(g * GROUP + first, GROUP - first)
        pltpu.make_async_copy(cells_in.at[at], cells_in.at[at], cell_sem.at[g]).wait()
        pltpu.make_async_copy(recv.at[at], recv.at[at], recv_sem.at[g]).wait()


    def absorb(g, carry):
        @pl.when(g == 0)
        def _():
            landed(0, 1)

        @pl.when(g > 0)
        def _():
            landed(g, 0)

        scatter(g)
        return carry

    def setup():
        loads[3].wait()
        loads[4].wait()
        for a in range(3):
            for b in range(3):
                wmat[a * C : (a + 1) * C, b * C : (b + 1) * C] = w_ref[a, b]
        acc[...] = jnp.zeros_like(acc)
        expand[...] = (iota((128, SPAN), 0).astype(F32) == within).astype(F32).astype(BF16)
        own = gx * 8 + gy
        recv[0] = pack(own)
        cells_in[0] = cell_tab[pl.ds(own, 1), :]

    def batch(g, carry):
        first = jnp.maximum(g * GROUP, 1)
        end = (g + 1) * GROUP

        def pack_and_send(i, carry):
            dest = partner(i)
            tile = dest[0] * 8 + dest[1]
            send[i] = pack(tile)
            cell_send[i] = cell_tab[pl.ds(tile, 1), :]

            @pl.when(i > first)
            def _():
                ship(i - 1)

            return carry

        lax.fori_loop(first, end, pack_and_send, 0)
        ship(end - 1)

        @pl.when(g == 0)
        def _():
            setup()

        @pl.when(g >= LAG)
        def _():
            absorb(g - LAG, 0)

        return carry

    lax.fori_loop(0, GROUPS, batch, 0)
    lax.fori_loop(GROUPS - LAG, GROUPS, absorb, 0)

    def settle(r):
        line = acc[r // 2, :, (r % 2) * C : (r % 2 + 1) * C]
        bev_ref[r] = line.astype(BF16)
        stage_col[0, r : r + 1, :] = line[0:1, :]
        stage_col[1, r : r + 1, :] = line[COLS - 1 : COLS, :]

    def halo(source, target, k, dx, dy):
        return pltpu.make_async_remote_copy(
            src_ref=source,
            dst_ref=target,
            send_sem=halo_send_sem.at[k],
            recv_sem=halo_sem.at[k],
            device_id=(gx + dx, gy + dy),
            device_id_type=MESH,
        )

    moves = [
        (bev_ref.at[0], bottom, -1, 0),
        (bev_ref.at[ROWS - 1], top, 1, 0),
        (col_send.at[0], col_recv.at[1], 0, -1),
        (col_send.at[1], col_recv.at[0], 0, 1),
        (corner_send.at[0], corner_recv.at[3], -1, -1),
        (corner_send.at[1], corner_recv.at[2], -1, 1),
        (corner_send.at[2], corner_recv.at[1], 1, -1),
        (corner_send.at[3], corner_recv.at[0], 1, 1),
    ]

    def inside(dx, dy):
        fine = jnp.logical_and(gx + dx >= 0, gx + dx < 16)
        return jnp.logical_and(fine, jnp.logical_and(gy + dy >= 0, gy + dy < 8))

    def launch(which):
        for k in which:
            source, target, dx, dy = moves[k]

            @pl.when(inside(dx, dy))
            def _(source=source, target=target, dx=dx, dy=dy, k=k):
                halo(source, target, k, dx, dy).start()

    settle(0)
    settle(ROWS - 1)
    for k in range(4):
        at = (ROWS - 1) * (k // 2)
        corner_send[k] = jnp.broadcast_to(stage_col[k % 2, at : at + 1, :], (16, C)).astype(BF16)
    for r in range(1, ROWS - 1):
        settle(r)
        if r == 2:
            launch((0, 1))
        if r == 6:
            launch((4, 5, 6, 7))
    col_send[0] = stage_col[0].astype(BF16)
    col_send[1] = stage_col[1].astype(BF16)
    bias = bias_ref[...]
    at = iota((COLS, C), 0)

    def finish(r, total):
        left = jnp.where(at == 0, 0.0, pltpu.roll(total[:, 0:C], 1, axis=0))
        right = jnp.where(at == COLS - 1, 0.0, pltpu.roll(total[:, 2 * C :], COLS - 1, axis=0))
        out = total[:, C : 2 * C] + left + right + bias
        edge_pre[0, r] = out[0:16]
        edge_pre[1, r] = out[COLS - 16 :]
        conv_ref[r] = jnp.maximum(out, 0.0).astype(BF16)

    launch((2, 3))

    def middle(m, carry):
        r = 2 * m + 1
        rows = [bev_ref[r - 1 + q] for q in range(4)]
        window = jnp.concatenate(
            [jnp.concatenate(rows[q : q + 2], axis=0) for q in range(3)], axis=1
        )
        total = jnp.dot(window, wmat[...], preferred_element_type=F32)
        finish(r, total[0:COLS])
        finish(r + 1, total[COLS:])
        return carry

    lax.fori_loop(0, ROWS // 2 - 1, middle, 0)

    for k, (source, target, dx, dy) in enumerate(moves):
        @pl.when(inside(-dx, -dy))
        def _(source=source, target=target, dx=dx, dy=dy, k=k):
            halo(source, target, k, -dx, -dy).wait_recv()

    window = jnp.concatenate(
        [
            jnp.concatenate([top[...], bev_ref[ROWS - 2]], axis=0),
            jnp.concatenate([bev_ref[0], bev_ref[ROWS - 1]], axis=0),
            jnp.concatenate([bev_ref[1], bottom[...]], axis=0),
        ],
        axis=1,
    )
    total = jnp.dot(window, wmat[...], preferred_element_type=F32)
    finish(0, total[0:COLS])
    finish(ROWS - 1, total[COLS:])
    for side in range(2):
        ext[0:1, :] = corner_recv[side].astype(F32)[0:1, :]
        ext[1:17, :] = col_recv[side].astype(F32)
        ext[17:18, :] = corner_recv[2 + side].astype(F32)[0:1, :]
        window = jnp.concatenate([ext[0:16, :], ext[1:17, :], ext[2:18, :]], axis=1).astype(BF16)
        edge[side] = jnp.dot(
            window, wmat[:, 2 * side * C : (2 * side + 1) * C], preferred_element_type=F32
        )
    small = iota((16, C), 0)
    for r in range(ROWS):
        left = edge_pre[0, r] + jnp.where(small == 0, edge[0, r : r + 1, :], 0.0)
        conv_ref[r, 0:16, :] = jnp.maximum(left, 0.0).astype(BF16)
        right = edge_pre[1, r] + jnp.where(small == 15, edge[1, r : r + 1, :], 0.0)
        conv_ref[r, COLS - 16 :, :] = jnp.maximum(right, 0.0).astype(BF16)

    for k, (source, target, dx, dy) in enumerate(moves):
        @pl.when(inside(dx, dy))
        def _(source=source, target=target, dx=dx, dy=dy, k=k):
            halo(source, target, k, dx, dy).wait_send()

    rest = pl.ds(1, DEV - 1)
    pltpu.make_async_copy(send.at[rest], send.at[rest], send_sem).wait()
    pltpu.make_async_copy(cell_send.at[rest], cell_send.at[rest], cell_send_sem).wait()


def shards(point_feats, point_tile, point_cell, point_count, conv_weight, conv_bias):
    smem = pl.BlockSpec(memory_space=pltpu.SMEM)
    vmem = pl.BlockSpec(memory_space=pltpu.VMEM)
    hbm = pl.BlockSpec(memory_space=pltpu.HBM)
    tile_map = pltpu.VMEM((ROWS, COLS, C), BF16)
    dma = pltpu.SemaphoreType.DMA
    return pl.pallas_call(
        main_kernel,
        name="exchange",
        out_shape=(tile_map, tile_map),
        in_specs=[hbm, hbm, smem, hbm, hbm, hbm],
        out_specs=(vmem, vmem),
        scratch_shapes=[
            pltpu.VMEM((POINTS // 128, 128), jnp.int32),
            pltpu.VMEM((POINTS // 128, 128), jnp.int32),
            pltpu.VMEM((3, 3, C, C), BF16),
            pltpu.VMEM((1, C), F32),
            pltpu.VMEM((POINTS, C), BF16),
            pltpu.VMEM((POINTS + 8, C), F32),
            pltpu.VMEM((DEV, CHUNK), BF16),
            pltpu.VMEM((256, CHUNK), BF16),
            pltpu.VMEM((DEV, 256), F32),
            pltpu.VMEM((DEV, 128), F32),
            pltpu.VMEM((DEV, 128), jnp.int32),
            pltpu.SMEM((DEV, 128), jnp.int32),
            pltpu.VMEM((DEV, 128), F32),
            pltpu.VMEM((DEV, 1, 128), F32),
            pltpu.VMEM((DEV, 1, 128), F32),
            pltpu.VMEM((CAP, C), F32),
            pltpu.VMEM((DEV, CAP, C), BF16),
            pltpu.VMEM((DEV, CAP, C), BF16),
            pltpu.VMEM((ROWS // 2, COLS, 2 * C), F32),
            pltpu.VMEM((128, SPAN), BF16),
            pltpu.VMEM((COLS, SPAN), BF16),
            pltpu.VMEM((SPAN, C), BF16),
            pltpu.VMEM((GROUP, 128), F32),
            pltpu.VMEM((3 * C, 3 * C), BF16),
            pltpu.VMEM((COLS, C), BF16),
            pltpu.VMEM((COLS, C), BF16),
            pltpu.VMEM((2, ROWS, C), BF16),
            pltpu.VMEM((2, ROWS, C), BF16),
            pltpu.VMEM((4, 16, C), BF16),
            pltpu.VMEM((4, 16, C), BF16),
            pltpu.VMEM((24, C), F32),
            pltpu.VMEM((2, ROWS, C), F32),
            pltpu.VMEM((2, ROWS, C), F32),
            pltpu.VMEM((2, ROWS, 16, C), F32),
            dma((5,)),
            dma,
            dma,
            dma((GROUPS,)),
            dma,
            dma((GROUPS,)),
            dma((8,)),
            dma((8,)),
        ],
        compiler_params=pltpu.CompilerParams(
            collective_id=0, has_side_effects=True, vmem_limit_bytes=64929792
        ),
    )(
        point_tile.reshape(POINTS // 128, 128),
        point_cell.reshape(POINTS // 128, 128),
        point_count,
        point_feats,
        conv_weight,
        conv_bias.reshape(1, C),
    )


def solution(mesh):
    in_specs = (
        P(("gx", "gy"), None),
        P(("gx", "gy"), None),
        P(("gx", "gy")),
        P(("gx", "gy")),
        P(),
        P(),
    )
    out_specs = (P("gx", "gy", None), P("gx", "gy", None))
    return jax.shard_map(shards, mesh=mesh, in_specs=in_specs, out_specs=out_specs, check_vma=False)
```
